32 devices in a mesh: member: 2 (over x), mp: 16 (over z, y, core).
Axes of the slice: x: 2, y: 2, z: 4, core: 2. Of those that a mesh axis runs over, the one named last changes fastest.
Arguments:
- nodes: bfloat16 [2048, 4096], P(('member', 'mp')), parts along dimension 0, may hold values from -6 to 6
- norm_gain: float32 [4096], replicated, may hold values from 0.1 to 1.9
- w_in: bfloat16 [4096, 16384], P(None, 'mp'), may hold values from -0.09375 to 0.09375
- b_in: float32 [16384], P('mp'), may hold values from -3 to 3
- w_out: bfloat16 [16384, 4096], P('mp'), may hold values from -0.046875 to 0.046875
- b_out: float32 [4096], replicated, may hold values from -3 to 3
Outputs:
- updated: bfloat16 [2048, 4096], P(('member', 'mp')), parts along dimension 0
The draws below stay inside these ranges and needn't reach their ends.
There are 2 independent parts, one for each index of `member`. The reference program is written for one: setup_inputs(seed, part) draws one part's arguments, and reference() takes and returns one part's arrays. A program takes and returns all parts, laid end to end along the dimension named above; an argument that names none is the same for every part. Nothing has to cross between parts.
All inputs are finite; a program needn't handle non-finite values.
Results may differ from the reference program's by a relative error of at most 0.015.
Values may be sent and summed in bfloat16 or wider, within the bound.
A program may use at most 128 MiB of HBM per device.

```python
import jax
import jax.numpy as jnp
from jax import lax

D = 4096
FF = 16384
ROWS = 1024
N_MP = 16


def levels(key, extent, pieces, low, high):
    loudness = 1.0
    for dim, blocks in pieces:
        draws = jax.random.uniform(jax.random.fold_in(jax.random.fold_in(key, 6), dim), (blocks,), jnp.float32, low / len(pieces), high / len(pieces))
        loudness = loudness * jnp.repeat(jnp.exp(draws), extent[dim] // blocks).reshape((-1,) + (1,) * (len(extent) - 1 - dim))
    return loudness


def gaussian(key, shape, deviation, limit, cuts=(), kind=jnp.bfloat16):
    drawn = deviation * jax.random.normal(key, shape, jnp.float32)
    if cuts:
        drawn = drawn * levels(key, shape, cuts, -0.22, 0.18)
    return jnp.clip(drawn, -limit, limit).astype(kind)


def setup_inputs(seed: int = 0, part: int = 0) -> dict:
    key_list = jax.random.split(jax.random.key(seed), 7)
    own_keys = jax.random.split(jax.random.fold_in(key_list[6], part), 7)
    return {
        "nodes": gaussian(own_keys[0], (ROWS, D), 1.0, 6.0, ((0, 16),)),
        "norm_gain": jnp.clip(1.0 + 0.18 * jax.random.normal(key_list[1], (D,), jnp.float32), 0.1, 1.9),
        "w_in": gaussian(key_list[2], (D, FF), D ** -0.5, 0.09375, ((1, 16),)),
        "b_in": gaussian(key_list[3], (FF,), 0.5, 3.0, ((0, 16),), jnp.float32),
        "w_out": gaussian(key_list[4], (FF, D), FF ** -0.5, 0.046875, ((0, 16),)),
        "b_out": gaussian(key_list[5], (D,), 0.5, 3.0, (), jnp.float32),
    }


def reference(nodes, norm_gain, w_in, b_in, w_out, b_out):
    values = nodes.astype(jnp.float32)
    mean = lax.optimization_barrier(jnp.mean(values, axis=1, keepdims=True))
    var = lax.optimization_barrier(jnp.mean((values - mean) ** 2, axis=1, keepdims=True))
    normed = ((values - mean) / jnp.sqrt(var + 1e-05) * norm_gain).astype(jnp.bfloat16)
    pre = jnp.dot(normed, w_in, preferred_element_type=jnp.float32) + b_in
    hidden = jax.nn.gelu(pre, approximate=True).astype(jnp.bfloat16)
    width = FF // N_MP

    def add_share(index, total):
        start = (index * width).astype(jnp.int32)
        left = lax.dynamic_slice_in_dim(hidden, start, width, 1)
        right = lax.dynamic_slice_in_dim(w_out, start, width, 0)
        share = jnp.dot(left, right, preferred_element_type=jnp.float32).astype(jnp.bfloat16)
        return total + share.astype(jnp.float32)
    mlp_out = lax.fori_loop(jnp.int32(0), jnp.int32(N_MP), add_share, jnp.zeros((nodes.shape[0], nodes.shape[1]), jnp.float32))
    return (values + mlp_out + b_out).astype(jnp.bfloat16)
```

```python
import functools

import jax
import jax.numpy as jnp
from jax import lax
from jax.experimental import pallas as pl
from jax.experimental.pallas import tpu as pltpu
from jax.sharding import PartitionSpec as P

MESH = pl.DeviceIdType.MESH
STRIP = 16
TILE = 256


def flip(value, bits):
    place = 1
    out = value
    while place <= bits:
        if bits & place:
            out = out + place - 2 * place * lax.rem(value // place, 2)
        place *= 2
    return out


def kernel(
    layers, nodes, gain, w_in_hbm, b_in, w_out_hbm, b_out, out,
    rows_all, w_in, w_out, hidden, part, from_core, from_y, from_z,
    w_sem, zs, zr, ys, yr, cs, cr, rcs, rcr, rys, ryr, rzs, rzr,
):
    m, d = nodes.shape
    f = w_in.shape[1]
    me = lax.axis_index("mp")
    a = me // 4
    b = lax.rem(me // 2, 2)
    c = lax.rem(me, 2)
    group = 4 * m

    def device(aa, bb, cc):
        return {"mp": aa * 4 + bb * 2 + cc}

    loads = [
        pltpu.make_async_copy(w_in_hbm, w_in, w_sem.at[0]),
        pltpu.make_async_copy(w_out_hbm, w_out, w_sem.at[1]),
    ]
    for load in loads:
        load.start()

    barrier = pltpu.get_barrier_semaphore()
    partners = [device(flip(a, j), b, c) for j in range(1, layers)]
    partners += [device(a, 1 - b, c), device(a, b, 1 - c)]
    for partner in partners:
        pl.semaphore_signal(barrier, inc=1, device_id=partner, device_id_type=MESH)

    def block(ref, aa, bb, cc):
        start = aa * group + (bb * 2 + cc) * m
        return ref.at[pl.ds(pl.multiple_of(start, m), m), :]

    mine = a * group + (b * 2 + c) * m

    def norm_strip(i, carry):
        at = pl.multiple_of(i * STRIP, STRIP)
        values = nodes[pl.ds(at, STRIP), :].astype(jnp.float32)
        mean = jnp.mean(values, axis=1, keepdims=True)
        var = jnp.mean((values - mean) ** 2, axis=1, keepdims=True)
        normed = (values - mean) / jnp.sqrt(var + 1e-05) * gain[...]
        rows_all[pl.ds(pl.multiple_of(mine + at, STRIP), STRIP), :] = normed.astype(
            jnp.bfloat16
        )
        return carry

    lax.fori_loop(0, m // STRIP, norm_strip, 0)
    pl.semaphore_wait(barrier, len(partners))

    sent = []

    def remote(src, dst, send, recv, target):
        return pltpu.make_async_remote_copy(
            src_ref=src, dst_ref=dst, send_sem=send, recv_sem=recv,
            device_id=target, device_id_type=MESH,
        )

    def send(*args):
        copy = remote(*args)
        copy.start()
        sent.append(copy)

    def arrived(dst, send_sem, recv_sem):
        remote(dst, dst, send_sem, recv_sem, device(a, b, 1 - c)).wait_recv()

    def gather_z(j):
        g = flip(a, j)
        own = block(rows_all, g, b, c)
        if j:
            arrived(own, zs.at[j], zr.at[j])
        send(own, own, ys.at[j], yr.at[j], device(a, 1 - b, c))
        send(own, own, cs.at[2 * j], cr.at[2 * j], device(a, b, 1 - c))

    def gather_y(j):
        g = flip(a, j)
        other = block(rows_all, g, 1 - b, c)
        arrived(other, ys.at[j], yr.at[j])
        send(other, other, cs.at[2 * j + 1], cr.at[2 * j + 1], device(a, b, 1 - c))

    def gather_c(j):
        g = flip(a, j)
        arrived(block(rows_all, g, b, 1 - c), cs.at[2 * j], cr.at[2 * j])
        arrived(block(rows_all, g, 1 - b, 1 - c), cs.at[2 * j + 1], cr.at[2 * j + 1])

    def compute(j):
        g = flip(a, j)
        rows = pl.ds(pl.multiple_of(g * group, group), group)

        def first(i, carry):
            cols = pl.ds(pl.multiple_of(i * TILE, TILE), TILE)
            pre = jnp.dot(
                rows_all[rows, :], w_in[:, cols], preferred_element_type=jnp.float32
            )
            pre = pre + b_in[:, cols]
            hidden[:, cols] = jax.nn.gelu(pre, approximate=True).astype(jnp.bfloat16)
            return carry

        def second(i, carry):
            cols = pl.ds(pl.multiple_of(i * TILE, TILE), TILE)
            share = jnp.dot(
                hidden[...], w_out[:, cols], preferred_element_type=jnp.float32
            )
            part[rows, cols] = share.astype(jnp.bfloat16)
            return carry

        if j == 0:
            loads[0].wait()
        lax.fori_loop(0, f // TILE, first, 0)
        if j == 0:
            loads[1].wait()
        lax.fori_loop(0, d // TILE, second, 0)
        for bb in range(2):
            send(
                block(part, g, bb, 1 - c), from_core.at[2 * j + bb],
                rcs.at[2 * j + bb], rcr.at[2 * j + bb], device(a, b, 1 - c),
            )

    def add(g, bb, landed):
        start = g * group + (bb * 2 + c) * m

        def strip(i, carry):
            at = pl.multiple_of(i * STRIP, STRIP)
            here = pl.ds(pl.multiple_of(start + at, STRIP), STRIP)
            total = part[here, :].astype(jnp.float32) + landed[
                pl.ds(at, STRIP), :
            ].astype(jnp.float32)
            part[here, :] = total.astype(jnp.bfloat16)
            return carry

        lax.fori_loop(0, m // STRIP, strip, 0)

    def reduce_c(j):
        g = flip(a, j)
        for bb in range(2):
            arrived(from_core.at[2 * j + bb], rcs.at[2 * j + bb], rcr.at[2 * j + bb])
        add(g, 1 - b, from_core.at[2 * j + 1 - b])
        send(
            block(part, g, 1 - b, c), from_y.at[j], rys.at[j], ryr.at[j],
            device(a, 1 - b, c),
        )
        add(g, b, from_core.at[2 * j + b])

    def reduce_y(j):
        g = flip(a, j)
        arrived(from_y.at[j], rys.at[j], ryr.at[j])
        add(g, b, from_y.at[j])
        if j:
            send(
                block(part, g, b, c), from_z.at[j], rzs.at[j], rzr.at[j],
                device(g, b, c),
            )

    own = block(rows_all, a, b, c)
    for j in range(1, layers):
        send(own, own, zs.at[j], zr.at[j], device(flip(a, j), b, c))
    gather_z(0)
    gather_y(0)
    if layers > 1:
        gather_z(1)
    for j in range(layers):
        gather_c(j)
        compute(j)
        if j >= 1:
            reduce_y(j - 1)
        if j + 1 < layers:
            gather_y(j + 1)
        if j + 2 < layers:
            gather_z(j + 2)
        reduce_c(j)
    reduce_y(layers - 1)
    for j in range(1, layers):
        arrived(from_z.at[j], rzs.at[j], rzr.at[j])

    def final(i, carry):
        at = pl.multiple_of(i * STRIP, STRIP)
        here = pl.ds(at, STRIP)
        total = part[pl.ds(pl.multiple_of(mine + at, STRIP), STRIP), :].astype(jnp.float32)
        for j in range(1, layers):
            total = total + from_z[j, here, :].astype(jnp.float32)
        total = nodes[here, :].astype(jnp.float32) + total + b_out[...]
        out[here, :] = total.astype(jnp.bfloat16)
        return carry

    lax.fori_loop(0, m // STRIP, final, 0)
    for copy in sent:
        copy.wait_send()


def solution(mesh):
    n = mesh.shape["mp"]
    layers = n // 4

    def local(nodes, norm_gain, w_in, b_in, w_out, b_out):
        m, d = nodes.shape
        f = w_in.shape[1]
        bf = jnp.bfloat16
        vmem = pl.BlockSpec(memory_space=pltpu.VMEM)
        hbm = pl.BlockSpec(memory_space=pl.ANY)
        dma = pltpu.SemaphoreType.DMA
        flops = 4 * n * m * d * f
        return pl.pallas_call(
            functools.partial(kernel, layers),
            out_shape=jax.ShapeDtypeStruct((m, d), bf),
            in_specs=[vmem, vmem, hbm, vmem, hbm, vmem],
            out_specs=vmem,
            scratch_shapes=[
                pltpu.VMEM((n * m, d), bf),
                pltpu.VMEM((d, f), bf),
                pltpu.VMEM((f, d), bf),
                pltpu.VMEM((4 * m, f), bf),
                pltpu.VMEM((n * m, d), bf),
                pltpu.VMEM((2 * layers, m, d), bf),
                pltpu.VMEM((layers, m, d), bf),
                pltpu.VMEM((layers, m, d), bf),
                dma((2,)),
                dma((layers,)), dma((layers,)),
                dma((layers,)), dma((layers,)),
                dma((2 * layers,)), dma((2 * layers,)),
                dma((2 * layers,)), dma((2 * layers,)),
                dma((layers,)), dma((layers,)),
                dma((layers,)), dma((layers,)),
            ],
            compiler_params=pltpu.CompilerParams(
                collective_id=0, has_side_effects=True, vmem_limit_bytes=67043328
            ),
            cost_estimate=pl.CostEstimate(
                flops=flops, bytes_accessed=4 * d * f, transcendentals=n * m * f
            ),
            name="ffn",
        )(nodes, norm_gain[None], w_in, b_in[None], w_out, b_out[None])

    return jax.shard_map(
        local,
        mesh=mesh,
        in_specs=(P(("member", "mp"), None), P(), P(None, "mp"), P("mp"), P("mp", None), P()),
        out_specs=P(("member", "mp"), None),
        check_vma=False,
    )
```

```python
import functools

import jax
import jax.numpy as jnp
from jax import lax
from jax.experimental import pallas as pl
from jax.experimental.pallas import tpu as pltpu
from jax.sharding import PartitionSpec as P

MESH = pl.DeviceIdType.MESH
STRIP = 16
TILE = 512
HALVES = 2


def flip(value, bits):
    place = 1
    out = value
    while place <= bits:
        if bits & place:
            out = out + place - 2 * place * lax.rem(value // place, 2)
        place *= 2
    return out


def kernel(
    layers, nodes, gain, w_in_hbm, b_in, w_out_hbm, b_out, out,
    rows_all, w_in, w_out, hidden, part, from_core, from_y, from_z,
    w_sem, zs, zr, qs, qr, ys, yr, cs, cr, rcs, rcr, rys, ryr, rzs, rzr,
):
    m, d = nodes.shape
    f = w_in.shape[1]
    me = lax.axis_index("mp")
    a = me // 4
    b = lax.rem(me // 2, 2)
    c = lax.rem(me, 2)
    group = 4 * m

    def device(aa, bb, cc):
        return {"mp": aa * 4 + bb * 2 + cc}

    loads = [
        pltpu.make_async_copy(w_in_hbm, w_in, w_sem.at[0]),
        pltpu.make_async_copy(w_out_hbm, w_out, w_sem.at[1]),
    ]
    for load in loads:
        load.start()

    barrier = pltpu.get_barrier_semaphore()
    partners = [device(flip(a, j), b, c) for j in range(1, layers)]
    partners += [device(a, 1 - b, c), device(a, b, 1 - c)]
    for partner in partners:
        pl.semaphore_signal(barrier, inc=1, device_id=partner, device_id_type=MESH)

    def block(ref, aa, bb, cc):
        start = aa * group + (bb * 2 + cc) * m
        return ref.at[pl.ds(pl.multiple_of(start, m), m), :]

    mine = a * group + (b * 2 + c) * m

    def norm_strip(i, carry):
        at = pl.multiple_of(i * STRIP, STRIP)
        values = nodes[pl.ds(at, STRIP), :].astype(jnp.float32)
        mean = jnp.mean(values, axis=1, keepdims=True)
        var = jnp.mean((values - mean) ** 2, axis=1, keepdims=True)
        normed = (values - mean) / jnp.sqrt(var + 1e-05) * gain[...]
        rows_all[pl.ds(pl.multiple_of(mine + at, STRIP), STRIP), :] = normed.astype(
            jnp.bfloat16
        )
        return carry

    lax.fori_loop(0, m // STRIP, norm_strip, 0)
    pl.semaphore_wait(barrier, len(partners))

    sent = []

    def remote(src, dst, send, recv, target):
        return pltpu.make_async_remote_copy(
            src_ref=src, dst_ref=dst, send_sem=send, recv_sem=recv,
            device_id=target, device_id_type=MESH,
        )

    def send(*args):
        copy = remote(*args)
        copy.start()
        sent.append(copy)

    def arrived(dst, send_sem, recv_sem):
        remote(dst, dst, send_sem, recv_sem, device(a, b, 1 - c)).wait_recv()

    early = m // 2
    late = m - early

    def xor(x, y):
        total, place = 0, 1
        while place < layers:
            total = total + place * lax.rem(x // place + y // place, 2)
            place *= 2
        return total

    mid = lax.rem((a + 1) // 2, 2) if layers == 4 else 0
    slots = list(range(layers))
    if layers == 4:
        slots[2], slots[3] = 2 + mid, 3 - mid
    groups = [xor(a, jj) for jj in slots]

    def late_rows(ref, aa, bb, cc):
        start = aa * group + (bb * 2 + cc) * m + early
        return ref.at[pl.ds(pl.multiple_of(start, STRIP), late), :]

    def early_rows(ref, aa, bb, cc):
        start = aa * group + (bb * 2 + cc) * m
        return ref.at[pl.ds(pl.multiple_of(start, STRIP), early), :]

    guarded = []

    def pass_on(p, rows, send_sems, recv_sems):
        g = groups[p]
        for step in (1, -1):
            if p == 0:
                sem = send_sems.at[0 if step == 1 else layers]
                ready = a < layers - 1 if step == 1 else a > 0
            else:
                sem = send_sems.at[slots[p]]
                ready = (
                    jnp.logical_and(g < a, a < layers - 1)
                    if step == 1
                    else jnp.logical_and(g > a, a > 0)
                )
            to = lax.rem(a + step + layers, layers)
            copy = remote(rows, rows, sem, recv_sems.at[xor(to, g)], device(to, b, c))

            @pl.when(ready)
            def _(copy=copy):
                copy.start()

            guarded.append((ready, copy))

    def gather_z(p):
        g, j = groups[p], slots[p]
        own = block(rows_all, g, b, c)
        if p:
            arrived(own, zs.at[j], zr.at[j])
            pass_on(p, own, zs, zr)
            first = early_rows(rows_all, g, b, c)
        else:
            pass_on(p, own, zs, zr)
            first = own
        send(first, first, ys.at[j], yr.at[j], device(a, 1 - b, c))
        send(own, own, cs.at[2 * j], cr.at[2 * j], device(a, b, 1 - c))

    def gather_q(p):
        g, j = groups[p], slots[p]
        rows = late_rows(rows_all, g, 1 - b, c)
        if p:
            arrived(rows, qs.at[j], qr.at[j])
        pass_on(p, rows, qs, qr)

    def gather_y(p):
        g, j = groups[p], slots[p]
        other = block(rows_all, g, 1 - b, c)
        if p:
            arrived(early_rows(rows_all, g, 1 - b, c), ys.at[j], yr.at[j])
        else:
            arrived(other, ys.at[j], yr.at[j])
        send(other, other, cs.at[2 * j + 1], cr.at[2 * j + 1], device(a, b, 1 - c))

    def gather_c(p):
        g, j = groups[p], slots[p]
        arrived(block(rows_all, g, b, 1 - c), cs.at[2 * j], cr.at[2 * j])
        arrived(block(rows_all, g, 1 - b, 1 - c), cs.at[2 * j + 1], cr.at[2 * j + 1])

    def compute(p):
        g, j = groups[p], slots[p]
        rows = pl.ds(pl.multiple_of(g * group, group), group)

        def first(i, carry):
            cols = pl.ds(pl.multiple_of(i * TILE, TILE), TILE)
            pre = jnp.dot(
                rows_all[rows, :], w_in[:, cols], preferred_element_type=jnp.float32
            )
            pre = pre + b_in[:, cols]
            hidden[:, cols] = jax.nn.gelu(pre, approximate=True).astype(jnp.bfloat16)
            return carry

        def second(i, carry):
            cols = pl.ds(pl.multiple_of(i * TILE, TILE), TILE)
            share = jnp.dot(
                hidden[...], w_out[:, cols], preferred_element_type=jnp.float32
            )
            part[rows, cols] = share.astype(jnp.bfloat16)
            return carry

        if p == 0:
            loads[0].wait()
        lax.fori_loop(0, f // TILE, first, 0)
        if p == 0:
            loads[1].wait()
        lax.fori_loop(0, d // TILE, second, 0)
        for bb in range(2):
            send(
                block(part, g, bb, 1 - c), from_core.at[2 * j + bb],
                rcs.at[2 * j + bb], rcr.at[2 * j + bb], device(a, b, 1 - c),
            )

    half = m // HALVES

    def piece(ref, aa, bb, cc, h):
        start = aa * group + (bb * 2 + cc) * m + h * half
        return ref.at[pl.ds(pl.multiple_of(start, half), half), :]

    def add(g, bb, landed, skip, count):
        start = g * group + (bb * 2 + c) * m + skip

        def strip(i, carry):
            at = pl.multiple_of(i * STRIP, STRIP)
            here = pl.ds(pl.multiple_of(start + at, STRIP), STRIP)
            total = part[here, :].astype(jnp.float32) + landed[
                pl.ds(at, STRIP), :
            ].astype(jnp.float32)
            part[here, :] = total.astype(jnp.bfloat16)
            return carry

        lax.fori_loop(0, count // STRIP, strip, 0)

    def reduce_c(p):
        g, j = groups[p], slots[p]
        for bb in range(2):
            arrived(from_core.at[2 * j + bb], rcs.at[2 * j + bb], rcr.at[2 * j + bb])
        add(g, 1 - b, from_core.at[2 * j + 1 - b], 0, m)

    def send_y(p):
        g, j = groups[p], slots[p]
        for h in range(HALVES):
            k = HALVES * j + h
            send(
                piece(part, g, 1 - b, c, h), from_y.at[j, pl.ds(h * half, half)],
                rys.at[k], ryr.at[k], device(a, 1 - b, c),
            )
        add(g, b, from_core.at[2 * j + b], 0, m)

    def reduce_y(p):
        g, j = groups[p], slots[p]
        for h in range(HALVES):
            k = HALVES * j + h
            landed = from_y.at[j, pl.ds(h * half, half)]
            arrived(landed, rys.at[k], ryr.at[k])
            add(g, b, landed, h * half, half)
            if p:
                send(
                    piece(part, g, b, c, h), from_z.at[j, pl.ds(h * half, half)],
                    rzs.at[k], rzr.at[k], device(g, b, c),
                )

    gather_z(0)
    gather_z(1)
    gather_y(0)
    gather_q(0)
    gather_c(0)
    compute(0)
    gather_z(2)
    reduce_c(0)
    send_y(0)
    gather_q(1)
    gather_y(1)
    for p in range(1, layers):
        if p + 2 < layers:
            gather_z(p + 2)
        if p + 1 < layers:
            gather_q(p + 1)
        gather_c(p)
        compute(p)
        reduce_c(p)
        if p != 1:
            send_y(p)
        if p == layers - 1:
            send_y(1)
        if p + 1 < layers:
            gather_y(p + 1)
        if p == 2:
            reduce_y(0)
        if p > 2:
            reduce_y(p - 1)
    reduce_y(layers - 1)
    reduce_y(1)
    for j in range(1, layers):
        for h in range(HALVES):
            k = HALVES * j + h
            arrived(from_z.at[j, pl.ds(h * half, half)], rzs.at[k], rzr.at[k])

    def final(i, carry):
        at = pl.multiple_of(i * STRIP, STRIP)
        here = pl.ds(at, STRIP)
        total = part[pl.ds(pl.multiple_of(mine + at, STRIP), STRIP), :].astype(jnp.float32)
        for j in range(1, layers):
            total = total + from_z[j, here, :].astype(jnp.float32)
        total = nodes[here, :].astype(jnp.float32) + total + b_out[...]
        out[here, :] = total.astype(jnp.bfloat16)
        return carry

    lax.fori_loop(0, m // STRIP, final, 0)
    for copy in sent:
        copy.wait_send()
    for ready, copy in guarded:

        @pl.when(ready)
        def _(copy=copy):
            copy.wait_send()


def solution(mesh):
    n = mesh.shape["mp"]
    layers = n // 4

    def local(nodes, norm_gain, w_in, b_in, w_out, b_out):
        m, d = nodes.shape
        f = w_in.shape[1]
        bf = jnp.bfloat16
        vmem = pl.BlockSpec(memory_space=pltpu.VMEM)
        hbm = pl.BlockSpec(memory_space=pl.ANY)
        dma = pltpu.SemaphoreType.DMA
        flops = 4 * n * m * d * f
        return pl.pallas_call(
            functools.partial(kernel, layers),
            out_shape=jax.ShapeDtypeStruct((m, d), bf),
            in_specs=[vmem, vmem, hbm, vmem, hbm, vmem],
            out_specs=vmem,
            scratch_shapes=[
                pltpu.VMEM((n * m, d), bf),
                pltpu.VMEM((d, f), bf),
                pltpu.VMEM((f, d), bf),
                pltpu.VMEM((4 * m, f), bf),
                pltpu.VMEM((n * m, d), bf),
                pltpu.VMEM((2 * layers, m, d), bf),
                pltpu.VMEM((layers, m, d), bf),
                pltpu.VMEM((layers, m, d), bf),
                dma((2,)),
                dma((layers + 1,)), dma((layers,)),
                dma((layers + 1,)), dma((layers,)),
                dma((layers,)), dma((layers,)),
                dma((2 * layers,)), dma((2 * layers,)),
                dma((2 * layers,)), dma((2 * layers,)),
                dma((HALVES * layers,)), dma((HALVES * layers,)),
                dma((HALVES * layers,)), dma((HALVES * layers,)),
            ],
            compiler_params=pltpu.CompilerParams(
                collective_id=0, has_side_effects=True, vmem_limit_bytes=67043328
            ),
            cost_estimate=pl.CostEstimate(
                flops=flops, bytes_accessed=4 * d * f, transcendentals=n * m * f
            ),
            name="ffn",
        )(nodes, norm_gain[None], w_in, b_in[None], w_out, b_out[None])

    return jax.shard_map(
        local,
        mesh=mesh,
        in_specs=(P(("member", "mp"), None), P(), P(None, "mp"), P("mp"), P("mp", None), P()),
        out_specs=P(("member", "mp"), None),
        check_vma=False,
    )
```
